128 devices in a mesh: left: 16 (over y, x_lo, core), right: 8 (over z, x_hi).
Axes of the slice: x: 4 (x_hi: 2, x_lo: 2; x = x_hi * 2 + x_lo), y: 4, z: 4, core: 2. Of those that a mesh axis runs over, the one named last changes fastest.
Arguments:
- tracer: float32 [2, 2048, 512, 256], P(None, None, 'left', 'right'), may hold values from -6 to 6
- symbol_x: float32 [2048], replicated, may hold values from 0.3 to 3
- symbol_y: float32 [512], replicated, may hold values from 0.3 to 3
- symbol_z: float32 [256], replicated, may hold values from 0.3 to 3
Outputs:
- modes: float32 [2, 2048, 512, 256], P(None, 'left', 'right')
The draws below stay inside these ranges and needn't reach their ends.
All inputs are finite; a program needn't handle non-finite values.
Results may differ from the reference program's by a relative error of at most 0.00007.
Values sent between devices are 32-bit elements; how exact they have to be, the bound alone decides.
A program may use at most 256 MiB of HBM per device.

```python
import jax
import jax.numpy as jnp
from jax import lax

GRID_X = 2048
GRID_Y = 512
GRID_Z = 256
FIELDS = 2


def level_of(stream_key, extent, shards, least, largest):
    def one(position, parts):
        draws = jax.random.uniform(jax.random.fold_in(jax.random.fold_in(stream_key, 6), position), (parts,), jnp.float32, least / len(shards), largest / len(shards))
        return jnp.repeat(jnp.exp(draws), extent[position] // parts).reshape((-1,) + (1,) * (len(extent) - position - 1))

    gain = one(*shards[0])
    for cut in shards[1:]:
        gain = gain * one(*cut)
    return gain


def normal_values(own_key, extent, scale, reach, shards=(), dtype=jnp.bfloat16):
    loudness = level_of(own_key, extent, shards, -0.22, 0.18) if shards else 1.0
    entries = jax.random.normal(own_key, extent, jnp.float32) * scale * loudness
    return jnp.minimum(jnp.maximum(entries, -reach), reach).astype(dtype)


def setup_inputs(seed: int = 0) -> dict:
    splits = jax.random.split(jax.random.key(seed), 5)
    return {
        "tracer": normal_values(splits[0], (FIELDS, GRID_X, GRID_Y, GRID_Z), 1.0, 6.0, ((2, 16), (3, 8)), jnp.float32),
        "symbol_x": jnp.clip(jax.random.uniform(splits[1], (GRID_X,), jnp.float32, 0.3, 3.0), 0.3, 3.0),
        "symbol_y": jnp.clip(jax.random.uniform(splits[2], (GRID_Y,), jnp.float32, 0.3, 3.0), 0.3, 3.0),
        "symbol_z": jnp.clip(jax.random.uniform(splits[3], (GRID_Z,), jnp.float32, 0.3, 3.0), 0.3, 3.0),
    }


def transform_table(count):
    rank = jnp.arange(count)
    angle = 2.0 * jnp.pi / count * (rank[:, None] * rank[None, :] % count).astype(jnp.float32)
    return (jnp.cos(angle) + jnp.sin(angle)) * count ** (-0.5)

def transform_dim(values, dim):
    moved = jnp.tensordot(values, transform_table(values.shape[dim]), axes=([dim], [0]), precision=lax.Precision.HIGHEST)
    return jnp.moveaxis(moved, -1, dim)

def reference(tracer, symbol_x, symbol_y, symbol_z):
    modes = tracer
    modes = transform_dim(modes, 1)
    modes = transform_dim(modes, 2)
    modes = transform_dim(modes, 3)
    symbol = symbol_x[:, None, None] + symbol_y[None, :, None] + symbol_z[None, None, :]
    modes = modes * lax.rsqrt(symbol)
    return modes
```

```python
import functools

import jax
import jax.numpy as jnp
import numpy as np
from jax import lax
from jax.experimental import pallas as pl
from jax.experimental.pallas import tpu as pltpu
from jax.sharding import PartitionSpec as P

MESH = pl.DeviceIdType.MESH
RADIX = 16
PAIRS = 8
LANES = 128
CHUNKS = 8
VMEM_BYTES = 67043328


def partner(pair):
    return (0, 8) if pair == 0 else (pair, RADIX - pair)


def split_bf16(table):
    high = table.astype(jnp.bfloat16)
    low = (table - high.astype(np.float32)).astype(jnp.bfloat16)
    return np.asarray(high), np.asarray(low)


def pair_blocks(count):
    inner = count // RADIX
    blocks = np.zeros((PAIRS, 2, 2, inner, inner), np.float64)
    i = np.arange(inner)[:, None]
    q = np.arange(inner)[None, :]
    for pair in range(PAIRS):
        ids = partner(pair)
        for half in range(2):
            angle = 2 * np.pi * ((i * (ids[half] + RADIX * q)) % count) / count
            if pair == 0:
                blocks[pair, half, half] = np.cos(angle) + np.sin(angle)
            else:
                blocks[pair, half, half] = np.cos(angle)
                blocks[pair, half, 1 - half] = np.sin(angle)
    return blocks / np.sqrt(count)


def stacked_tables(table):
    high, low = split_bf16(table.astype(np.float32))
    return np.concatenate([high, low], axis=1)


def x_tables():
    blocks = pair_blocks(2048)
    q = blocks.reshape(PAIRS, 2, 2, 128, 16, 8)
    rows = np.transpose(q, (0, 4, 1, 5, 2, 3))
    return stacked_tables(rows.reshape(PAIRS, 256, 256))


def y_tables():
    blocks = pair_blocks(512)
    v = blocks.reshape(PAIRS, 2, 2, 32, 8, 4)
    full = np.einsum("pabrdv,jk->pdvjabrk", v, np.eye(4))
    return stacked_tables(full.reshape(PAIRS, 256, 256))


def z_table():
    src, zc, j = np.meshgrid(np.arange(8), np.arange(8), np.arange(4), indexing="ij")
    z = (32 * src + 8 * j + zc).reshape(-1)
    k = np.arange(256)
    angle = 2 * np.pi * ((z[:, None] * k[None, :]) % 256) / 256
    table = ((np.cos(angle) + np.sin(angle)) / 16.0).astype(np.float32)
    high, low = split_bf16(table)
    return np.stack([high, low])


def small_hartley(v):
    n = len(v)
    if n == 1:
        return v
    half = n // 2
    even = small_hartley(v[0::2])
    odd = small_hartley(v[1::2])
    out = [None] * n
    for k in range(half):
        c = float(np.cos(2 * np.pi * k / n))
        s = float(np.sin(2 * np.pi * k / n))
        back = odd[-k % half]
        if k == 0:
            turned = odd[0]
        elif 4 * k == n:
            turned = back
        elif 8 * k == n:
            turned = (odd[k] + back) * c
        elif 8 * k == 3 * n:
            turned = (back - odd[k]) * s
        else:
            turned = odd[k] * c + back * s
        out[k] = even[k] + turned
        out[k + half] = even[k] - turned
    return out


NT = (((1,), (1,)), ((), ()))
TN = (((0,), (0,)), ((), ()))


def radix_step(load, high_ref, low_ref):
    def rows(t, carry):
        zz, g = t // 8, t % 8
        parts = small_hartley(load(zz, g))
        at = pl.ds(pl.multiple_of(zz * 128 + g * 16, 16), 16)
        for pair in range(PAIRS):
            for half, p in enumerate(partner(pair)):
                value = parts[p]
                high = value.astype(jnp.bfloat16)
                low = (value - high.astype(jnp.float32)).astype(jnp.bfloat16)
                lanes = slice(half * LANES, (half + 1) * LANES)
                high_ref[pair, at, lanes] = high
                low_ref[pair, at, lanes] = low
        return carry

    lax.fori_loop(0, 16, rows, 0)


def matmul_step(table_ref, high_ref, low_ref, store):
    def one(pair, carry):
        high = high_ref[pair]
        table = table_ref[pair]
        both = lax.dot_general(table, high, NT, preferred_element_type=jnp.float32)
        rest = lax.dot_general(table[:256], low_ref[pair], NT, preferred_element_type=jnp.float32)
        store(pair, both[:256] + both[256:] + rest)
        return carry

    lax.fori_loop(0, PAIRS, one, 0)


def exchange_kernel(
    x_hbm, wx_hbm, wy_hbm, l_hbm, r_hbm,
    x_ref, wx_ref, wy_ref, xo_ref, lb_ref, yo_ref, high_ref, low_ref,
    load_sem, table_sem, fetch_sem,
    l_send, l_recv, l_own, r_send, r_recv, r_own,
):
    left = lax.axis_index("left")
    right = lax.axis_index("right")

    def left_peer(o):
        return (lax.rem(left + o, 16), right)

    def right_peer(o):
        return (left, lax.rem(right + o, 8))

    def x_load(f, a):
        lanes = pl.ds(pl.multiple_of(a * LANES, LANES), LANES)
        return pltpu.make_async_copy(x_hbm.at[f, :, lanes], x_ref.at[a], load_sem.at[a])

    def x_start(f):
        def one(a, carry):
            x_load(f, a).start()
            return carry

        lax.fori_loop(0, RADIX, one, 0)

    def x_wait(f):
        def one(a, carry):
            x_load(f, a).wait()
            return carry

        lax.fori_loop(0, RADIX, one, 0)

    def wx_load():
        return pltpu.make_async_copy(wx_hbm, wx_ref, table_sem.at[0])

    def wy_load():
        return pltpu.make_async_copy(wy_hbm, wy_ref, table_sem.at[1])

    x_start(0)
    wx_load().start()

    barrier = pltpu.get_barrier_semaphore()

    def greet_left(o, carry):
        pl.semaphore_signal(barrier, inc=1, device_id=left_peer(o), device_id_type=MESH)
        return carry

    def greet_right(o, carry):
        pl.semaphore_signal(barrier, inc=1, device_id=right_peer(o), device_id_type=MESH)
        return carry

    lax.fori_loop(1, 16, greet_left, 0)
    lax.fori_loop(1, 8, greet_right, 0)
    pl.semaphore_wait(barrier, 22)

    def l_copy(c, o):
        to = lax.rem(left + o, 16)
        return pltpu.make_async_remote_copy(
            src_ref=xo_ref.at[c, to],
            dst_ref=l_hbm.at[c, left],
            send_sem=l_send.at[c, o],
            recv_sem=l_recv.at[c, o],
            device_id=(to, right),
            device_id_type=MESH,
        )

    def l_keep(c):
        return pltpu.make_async_copy(xo_ref.at[c, left], l_hbm.at[c, left], l_own.at[c])

    def r_copy(c, o):
        to = lax.rem(right + o, 8)
        rows = pl.ds(pl.multiple_of((c % 4) * 16, 16), 16)
        return pltpu.make_async_remote_copy(
            src_ref=yo_ref.at[c, to],
            dst_ref=r_hbm.at[right, c // 4, :, rows],
            send_sem=r_send.at[c, o],
            recv_sem=r_recv.at[c, o],
            device_id=(left, to),
            device_id_type=MESH,
        )

    def r_keep(c):
        rows = pl.ds(pl.multiple_of((c % 4) * 16, 16), 16)
        return pltpu.make_async_copy(yo_ref.at[c, right], r_hbm.at[right, c // 4, :, rows], r_own.at[c])

    wx_load().wait()

    def x_chunk(c, carry):
        @pl.when(c == 0)
        def _():
            x_wait(0)
            wy_load().start()

        @pl.when(c == 4)
        def _():
            x_start(1)
            x_wait(1)

        first = (c % 4) * 2

        def load(zz, g):
            rows = pl.ds(g * 128 + first + zz, 16, stride=8)
            return [x_ref[a, rows, :] for a in range(RADIX)]

        def store(pair, value):
            at = pl.ds(pl.multiple_of(pair * 16, 16), 16)
            for zz in range(2):
                xo_ref[c, :, zz, at, :] = value[:, zz * LANES : (zz + 1) * LANES].reshape(16, 16, LANES)

        radix_step(load, high_ref, low_ref)
        matmul_step(wx_ref, high_ref, low_ref, store)

        def send(o, carry):
            l_copy(c, o).start()
            return carry

        lax.fori_loop(1, 16, send, 0)
        l_keep(c).start()
        return carry

    lax.fori_loop(0, CHUNKS, x_chunk, 0)
    wy_load().wait()

    def y_chunk(c, carry):
        def arrive(o, carry):
            l_copy(c, o).wait_recv()
            return carry

        l_keep(c).wait()
        lax.fori_loop(1, 16, arrive, 0)
        fetch = pltpu.make_async_copy(l_hbm.at[c], lb_ref, fetch_sem)
        fetch.start()
        fetch.wait()

        def load(zz, g):
            rows = pl.ds(pl.multiple_of(g * 16, 16), 16)
            return [lb_ref[s, zz, rows, :] for s in range(RADIX)]

        def store(pair, value):
            at = pl.ds(pl.multiple_of(pair * 4, 4), 4)
            for zz in range(2):
                yo_ref[c, :, at, zz * 8 : (zz + 1) * 8, :] = value[:, zz * LANES : (zz + 1) * LANES].reshape(
                    8, 4, 8, LANES
                )

        radix_step(load, high_ref, low_ref)
        matmul_step(wy_ref, high_ref, low_ref, store)

        def send(o, carry):
            r_copy(c, o).start()
            return carry

        lax.fori_loop(1, 8, send, 0)
        r_keep(c).start()
        return carry

    lax.fori_loop(0, CHUNKS, y_chunk, 0)

    def finish(c, carry):
        def l_done(o, carry):
            l_copy(c, o).wait_send()
            return carry

        def r_done(o, carry):
            r_copy(c, o).wait()
            return carry

        lax.fori_loop(1, 16, l_done, 0)
        lax.fori_loop(1, 8, r_done, 0)
        r_keep(c).wait()
        return carry

    lax.fori_loop(0, CHUNKS, finish, 0)


def exchange(x, wx, wy):
    f32 = jnp.float32
    dma = pltpu.SemaphoreType.DMA
    hbm = pl.BlockSpec(memory_space=pltpu.HBM)
    _, r = pl.pallas_call(
        exchange_kernel,
        out_shape=(
            jax.ShapeDtypeStruct((CHUNKS, 16, 2, 128, LANES), f32),
            jax.ShapeDtypeStruct((8, 2, 32, 64, LANES), f32),
        ),
        in_specs=[hbm] * 3,
        out_specs=(hbm, hbm),
        scratch_shapes=[
            pltpu.VMEM((RADIX, 1024, LANES), f32),
            pltpu.VMEM((PAIRS, 512, 256), jnp.bfloat16),
            pltpu.VMEM((PAIRS, 512, 256), jnp.bfloat16),
            pltpu.VMEM((CHUNKS, 16, 2, 128, LANES), f32),
            pltpu.VMEM((16, 2, 128, LANES), f32),
            pltpu.VMEM((CHUNKS, 8, 32, 16, LANES), f32),
            pltpu.VMEM((PAIRS, 256, 256), jnp.bfloat16),
            pltpu.VMEM((PAIRS, 256, 256), jnp.bfloat16),
            dma((RADIX,)),
            dma((2,)),
            dma,
            dma((CHUNKS, 16)),
            dma((CHUNKS, 16)),
            dma((CHUNKS,)),
            dma((CHUNKS, 8)),
            dma((CHUNKS, 8)),
            dma((CHUNKS,)),
        ],
        compiler_params=pltpu.CompilerParams(
            collective_id=0, has_side_effects=True, vmem_limit_bytes=VMEM_BYTES
        ),
        name="exchange",
    )(x, wx, wy)
    return r


def last_kernel(sy_ref, r_ref, h_ref, sx_ref, sz_ref, o_hbm, o_ref, high_ref, low_ref, base_ref, o_sem):
    step = pl.program_id(0)
    vlo = step % 4
    slot = step % 2

    def out_copy(at_step, lane):
        where = at_step % 2
        return pltpu.make_async_copy(
            o_ref.at[where, lane],
            o_hbm.at[at_step // 4, :, pl.ds(pl.multiple_of(at_step % 4 * 16, 16), 16), pl.ds(lane * LANES, LANES)],
            o_sem.at[where, lane],
        )

    base_ref[...] = sx_ref[...] + sz_ref[...]
    for pair in range(PAIRS):
        for half, u in enumerate(partner(pair)):
            rows = [r_ref[src, 0, pair, 0, pl.ds(half, 32, stride=2), :] for src in range(8)]
            value = jnp.concatenate(rows, axis=0)
            high = value.astype(jnp.bfloat16)
            low = (value - high.astype(jnp.float32)).astype(jnp.bfloat16)
            high_ref[:, u * LANES : (u + 1) * LANES] = high
            low_ref[:, u * LANES : (u + 1) * LANES] = low

    @pl.when(step >= 2)
    def _():
        for lane in range(2):
            out_copy(step - 2, lane).wait()

    def some(t, carry):
        at = pl.ds(pl.multiple_of(t * 512, 512), 512)
        high = high_ref[:, at]
        acc = lax.dot_general(high, h_ref[0], TN, preferred_element_type=jnp.float32)
        acc += lax.dot_general(high, h_ref[1], TN, preferred_element_type=jnp.float32)
        acc += lax.dot_general(low_ref[:, at], h_ref[0], TN, preferred_element_type=jnp.float32)
        for i in range(4):
            u = t * 4 + i
            scale = lax.rsqrt(base_ref[...] + sy_ref[vlo * 16 + u])
            value = acc[i * 128 : (i + 1) * 128] * scale
            for lane in range(2):
                flat = o_ref.at[slot, lane].reshape(2048, LANES)
                for pair in range(PAIRS):
                    for half, p in enumerate(partner(pair)):
                        at_row = pair * 16 + half * 8
                        flat[pl.ds(p * 16 + u, 8, stride=256), :] = value[
                            at_row : at_row + 8, lane * LANES : (lane + 1) * LANES
                        ]
        return carry

    lax.fori_loop(0, 4, some, 0)
    for lane in range(2):
        out_copy(step, lane).start()

    @pl.when(step == 7)
    def _():
        for lane in range(2):
            out_copy(step - 1, lane).wait()
            out_copy(step, lane).wait()


def last(r, h, sx, sy, sz):
    f32 = jnp.float32
    return pl.pallas_call(
        last_kernel,
        grid=(8,),
        out_shape=jax.ShapeDtypeStruct((2, 128, 64, 256), f32),
        in_specs=[
            pl.BlockSpec(memory_space=pltpu.SMEM),
            pl.BlockSpec((8, 1, 8, 1, 64, LANES), lambda i: (0, i // 4, 0, i % 4, 0, 0)),
            pl.BlockSpec((2, 256, 256), lambda i: (0, 0, 0)),
            pl.BlockSpec((128, 1), lambda i: (0, 0)),
            pl.BlockSpec((1, 256), lambda i: (0, 0)),
        ],
        out_specs=pl.BlockSpec(memory_space=pltpu.HBM),
        scratch_shapes=[
            pltpu.VMEM((2, 2, 128, 16, LANES), f32),
            pltpu.VMEM((256, 2048), jnp.bfloat16),
            pltpu.VMEM((256, 2048), jnp.bfloat16),
            pltpu.VMEM((128, 256), f32),
            pltpu.SemaphoreType.DMA((2, 2)),
        ],
        compiler_params=pltpu.CompilerParams(vmem_limit_bytes=VMEM_BYTES),
        name="last",
    )(sy, r.reshape(8, 2, 8, 4, 64, LANES), h, sx, sz)


def local(tracer, symbol_x, symbol_y, symbol_z):
    x = jnp.transpose(tracer, (0, 2, 3, 1)).reshape(2, 1024, 2048)
    r = exchange(x, x_tables(), y_tables())
    part_x = lax.dynamic_slice_in_dim(symbol_x, lax.axis_index("left") * 128, 128)
    part_y = lax.dynamic_slice_in_dim(symbol_y, lax.axis_index("right") * 64, 64)
    sx = part_x.reshape(8, 16).T[np.asarray([p for pair in range(PAIRS) for p in partner(pair)])].reshape(128, 1)
    return last(r, z_table(), sx, part_y, symbol_z.reshape(1, 256))


def solution(mesh):
    in_specs = (P(None, None, "left", "right"), P(), P(), P())
    out_specs = P(None, "left", "right", None)
    return jax.shard_map(local, mesh=mesh, in_specs=in_specs, out_specs=out_specs, check_vma=False)
```

```python
import jax
import jax.numpy as jnp
import numpy as np
from jax import lax
from jax.experimental import pallas as pl
from jax.experimental.pallas import tpu as pltpu
from jax.sharding import PartitionSpec as P

MESH = pl.DeviceIdType.MESH
RADIX = 16
PAIRS = 8
LANES = 128
CHUNKS = 8
VMEM_BYTES = 46 * 2**20
PITCH = 136
UNROLL = 2


def partner(pair):
    return (0, 8) if pair == 0 else (pair, RADIX - pair)


def split_bf16(table):
    high = table.astype(jnp.bfloat16)
    low = (table - high.astype(np.float32)).astype(jnp.bfloat16)
    return np.asarray(high), np.asarray(low)


def pair_blocks(count):
    inner = count // RADIX
    blocks = np.zeros((PAIRS, 2, 2, inner, inner), np.float64)
    i = np.arange(inner)[:, None]
    q = np.arange(inner)[None, :]
    for pair in range(PAIRS):
        ids = partner(pair)
        for half in range(2):
            angle = 2 * np.pi * ((i * (ids[half] + RADIX * q)) % count) / count
            if pair == 0:
                blocks[pair, half, half] = np.cos(angle) + np.sin(angle)
            else:
                blocks[pair, half, half] = np.cos(angle)
                blocks[pair, half, 1 - half] = np.sin(angle)
    return blocks / np.sqrt(count)


def stacked_tables(table):
    high, low = split_bf16(table.astype(np.float32))
    return np.concatenate([high, low], axis=1)


def x_tables():
    blocks = pair_blocks(2048)
    q = blocks.reshape(PAIRS, 2, 2, 128, 16, 8)
    rows = np.transpose(q, (0, 4, 1, 5, 2, 3))
    return stacked_tables(rows.reshape(PAIRS, 256, 256))


def y_tables():
    blocks = pair_blocks(512)
    v = blocks.reshape(PAIRS, 2, 2, 32, 8, 4)
    full = np.einsum("pabrdv,jk->pdvjabrk", v, np.eye(4))
    return stacked_tables(full.reshape(PAIRS, 256, 256))


def z_table():
    src, zc, j = np.meshgrid(np.arange(8), np.arange(8), np.arange(4), indexing="ij")
    z = (32 * src + 8 * j + zc).reshape(-1)
    k = np.arange(256)
    angle = 2 * np.pi * ((z[:, None] * k[None, :]) % 256) / 256
    table = ((np.cos(angle) + np.sin(angle)) / 16.0).astype(np.float32)
    high, low = split_bf16(table)
    return np.concatenate([high, low], axis=1)


def small_hartley(v):
    n = len(v)
    if n == 1:
        return v
    half = n // 2
    even = small_hartley(v[0::2])
    odd = small_hartley(v[1::2])
    out = [None] * n
    for k in range(half):
        c = float(np.cos(2 * np.pi * k / n))
        s = float(np.sin(2 * np.pi * k / n))
        back = odd[-k % half]
        if k == 0:
            turned = odd[0]
        elif 4 * k == n:
            turned = back
        elif 8 * k == n:
            turned = (odd[k] + back) * c
        elif 8 * k == 3 * n:
            turned = (back - odd[k]) * s
        else:
            turned = odd[k] * c + back * s
        out[k] = even[k] + turned
        out[k + half] = even[k] - turned
    return out


NT = (((1,), (1,)), ((), ()))
TN = (((0,), (0,)), ((), ()))


def radix_step(load, high_ref, low_ref):
    def rows(t, carry):
        zz, g = t // 8, t % 8
        parts = small_hartley(load(zz, g))
        at = pl.ds(pl.multiple_of(zz * 128 + g * 16, 16), 16)
        for pair in range(PAIRS):
            for half, p in enumerate(partner(pair)):
                value = parts[p]
                high = value.astype(jnp.bfloat16)
                low = (value - high.astype(jnp.float32)).astype(jnp.bfloat16)
                lanes = slice(half * LANES, (half + 1) * LANES)
                high_ref[pair, at, lanes] = high
                low_ref[pair, at, lanes] = low
        return carry

    lax.fori_loop(0, 16, rows, 0)


def matmul_step(table_ref, high_ref, low_ref, store):
    def some(i, carry):
        for j in range(UNROLL):
            pair = i * UNROLL + j
            table = table_ref[pair]
            both = lax.dot_general(table, high_ref[pair], NT, preferred_element_type=jnp.float32)
            rest = lax.dot_general(table[:256], low_ref[pair], NT, preferred_element_type=jnp.float32)
            store(pair, both[:256] + both[256:] + rest)
        return carry

    lax.fori_loop(0, PAIRS // UNROLL, some, 0)


def transform_kernel(
    x_hbm, wx_hbm, wy_hbm, h_hbm, sx_hbm, sy_hbm, sz_hbm, l_hbm, r_hbm, o_ref,
    x_ref, wx_ref, wy_ref, h_ref, sx_ref, sy_ref, sz_ref, xo_ref, lb_ref, zb_ref, zt_ref, high_ref, low_ref,
    stage_ref, base_ref, turn_ref,
    load_sem, table_sem, fetch_sem, zb_sem, zt_sem,
    l_send, l_recv, l_own, r_send, r_recv, r_own, tail_send, tail_recv,
):
    left = lax.axis_index("left")
    right = lax.axis_index("right")

    def left_to(o):
        m = 16 - o
        dx, dy, dc = m // 8, m // 2 % 4, m % 2
        return lax.rem(left // 4 + dy, 4) * 4 + lax.rem(left // 2 + dx, 2) * 2 + lax.rem(left + dc, 2)

    def right_to(o):
        m = 8 - o
        dx, dz = m // 4, m % 4
        return lax.rem(right // 2 + dz, 4) * 2 + lax.rem(right + dx, 2)

    def each(first, last, action):
        def one(i, carry):
            action(i)
            return carry

        lax.fori_loop(first, last, one, 0)

    def x_load(f, g, a):
        rows = pl.ds(pl.multiple_of(g * LANES, LANES), LANES)
        lanes = pl.ds(pl.multiple_of(a * LANES, LANES), LANES)
        return pltpu.make_async_copy(x_hbm.at[f, rows, lanes], x_ref.at[a, rows], load_sem.at[g, a])

    def x_start(f):
        each(0, 8, lambda g: each(0, RADIX, lambda a: x_load(f, g, a).start()))

    wx_load = pltpu.make_async_copy(wx_hbm, wx_ref, table_sem.at[0])
    other_loads = [
        pltpu.make_async_copy(source, target, table_sem.at[1 + i])
        for i, (source, target) in enumerate(
            ((wy_hbm, wy_ref), (h_hbm, h_ref), (sx_hbm, sx_ref), (sy_hbm, sy_ref), (sz_hbm, sz_ref))
        )
    ]

    x_start(0)
    wx_load.start()

    barrier = pltpu.get_barrier_semaphore()

    def greet(device):
        pl.semaphore_signal(barrier, inc=1, device_id=device, device_id_type=MESH)

    each(1, 16, lambda o: greet((left_to(o), right)))
    each(1, 8, lambda o: greet((left, right_to(o))))
    pl.semaphore_wait(barrier, 22)
    for load in other_loads:
        load.start()

    def l_copy(c, o):
        to = left_to(o)
        return pltpu.make_async_remote_copy(
            src_ref=xo_ref.at[c, to],
            dst_ref=l_hbm.at[c, left],
            send_sem=l_send.at[c, o],
            recv_sem=l_recv.at[c, o],
            device_id=(to, right),
            device_id_type=MESH,
        )

    def l_keep(c):
        return pltpu.make_async_copy(xo_ref.at[c, left], l_hbm.at[c, left], l_own.at[c])

    yo_ref = xo_ref.reshape(CHUNKS, 8, 4, PAIRS, 16, LANES)

    def r_rows(c):
        return pl.ds(pl.multiple_of((c % 4) * 16, 16), 16)

    def r_copy(c, o):
        to = right_to(o)
        return pltpu.make_async_remote_copy(
            src_ref=yo_ref.at[c, to],
            dst_ref=r_hbm.at[right, c // 4, :, :, r_rows(c)],
            send_sem=r_send.at[c, o],
            recv_sem=r_recv.at[c, o],
            device_id=(left, to),
            device_id_type=MESH,
        )

    def r_keep(c):
        return pltpu.make_async_copy(
            yo_ref.at[c, right], r_hbm.at[right, c // 4, :, :, r_rows(c)], r_own.at[c]
        )

    def tail_copy(v, o):
        to = right_to(o)
        return pltpu.make_async_remote_copy(
            src_ref=yo_ref.at[CHUNKS - 1, to, v],
            dst_ref=zt_ref.at[1, right, v],
            send_sem=tail_send.at[v, o],
            recv_sem=tail_recv.at[v, o],
            device_id=(left, to),
            device_id_type=MESH,
        )

    def x_chunk(c, carry):
        @pl.when(c == 4)
        def _():
            x_start(1)

        first = (c % 4) * 2

        def load(zz, g):
            @pl.when((c % 4 == 0) & (zz == 0))
            def _():
                each(0, RADIX, lambda a: x_load(c // 4, g, a).wait())

            rows = pl.ds(g * LANES + first + zz, 16, stride=8)
            return [x_ref[a, rows, :] for a in range(RADIX)]

        def store(pair, value):
            at = pl.ds(pl.multiple_of(pair * 16, 16), 16)
            for zz in range(2):
                xo_ref[c, :, zz, at, :] = value[:, zz * LANES : (zz + 1) * LANES].reshape(16, 16, LANES)

        radix_step(load, high_ref, low_ref)

        @pl.when(c == 0)
        def _():
            wx_load.wait()

        matmul_step(wx_ref, high_ref, low_ref, store)
        each(1, 16, lambda o: l_copy(c, o).start())
        l_keep(c).start()
        return carry

    lax.fori_loop(0, CHUNKS, x_chunk, 0)
    for load in other_loads:
        load.wait()

    turn_ref[...] = jnp.transpose(jnp.broadcast_to(sx_ref[pl.ds(left, 1), :], (LANES, LANES)))
    for pair in range(PAIRS):
        for half, p in enumerate(partner(pair)):
            at = pair * 16 + half * 8
            column = turn_ref[pl.ds(p, 8, stride=16), :]
            for lane in range(2):
                lanes = slice(lane * LANES, (lane + 1) * LANES)
                base_ref[at : at + 8, lanes] = column + sz_ref[:, lanes]

    def y_chunk(c, carry):
        l_keep(c).wait()
        each(1, 16, lambda o: l_copy(c, o).wait_recv())
        fetch = pltpu.make_async_copy(l_hbm.at[c], lb_ref, fetch_sem)
        fetch.start()
        each(1, 16, lambda o: l_copy(c, o).wait_send())
        fetch.wait()

        def load(zz, g):
            rows = pl.ds(pl.multiple_of(g * 16, 16), 16)
            return [lb_ref[s, zz, rows, :] for s in range(RADIX)]

        def store(pair, value):
            for zz in range(2):
                yo_ref[c, :, :, pair, zz * 8 : (zz + 1) * 8, :] = value[:, zz * LANES : (zz + 1) * LANES].reshape(
                    8, 4, 8, LANES
                )

        radix_step(load, high_ref, low_ref)
        matmul_step(wy_ref, high_ref, low_ref, store)

        @pl.when(c < CHUNKS - 1)
        def _():
            each(1, 8, lambda o: r_copy(c, o).start())
            r_keep(c).start()

        return carry

    lax.fori_loop(0, CHUNKS, y_chunk, 0)
    each(0, 4, lambda v: each(1, 8, lambda o: tail_copy(v, o).start()))
    zt_ref[1, right] = yo_ref[CHUNKS - 1, right]

    def r_arrived(c):
        each(1, 8, lambda o: r_copy(c, o).wait_recv())
        r_keep(c).wait()

    def zb_fetch(unit):
        slot = unit % 2
        return pltpu.make_async_copy(
            r_hbm.at[:, unit // 4, unit % 4, :, 0:48], zb_ref.at[slot], zb_sem.at[slot]
        )

    zt_fetch = pltpu.make_async_copy(r_hbm.at[:, 0, :, :, 48:64], zt_ref.at[0], zt_sem)

    def z_unit(unit):
        f, v, slot = unit // 4, unit % 4, unit % 2
        for pair in range(PAIRS):
            for half, u in enumerate(partner(pair)):
                rows = []
                for src in range(8):
                    rows.append(zb_ref[slot, src, pair, pl.ds(half, 24, stride=2), :])
                    rows.append(zt_ref[f, src, v, pair, pl.ds(half, 8, stride=2), :])
                value = jnp.concatenate(rows, axis=0)
                high = value.astype(jnp.bfloat16)
                low = (value - high.astype(jnp.float32)).astype(jnp.bfloat16)
                lanes = slice(u % 2 * LANES, (u % 2 + 1) * LANES)
                high_ref[u // 2, :, lanes] = high
                low_ref[u // 2, :, lanes] = low

        def some(t, carry):
            both = lax.dot_general(high_ref[t], h_ref[...], TN, preferred_element_type=jnp.float32)
            rest = lax.dot_general(low_ref[t], h_ref[:, :256], TN, preferred_element_type=jnp.float32)
            acc = both[:, :256] + both[:, 256:] + rest
            for i in range(2):
                u = t * 2 + i
                scale = lax.rsqrt(base_ref[...] + sy_ref[right * 64 + v * 16 + u])
                value = acc[i * LANES : (i + 1) * LANES] * scale
                for lane in range(2):
                    at = pl.ds(pl.multiple_of(u * PITCH, 8), LANES)
                    stage_ref[lane, at, :] = value[:, lane * LANES : (lane + 1) * LANES]
            return carry

        lax.fori_loop(0, PAIRS, some, 0)

        def out_rows(q, carry):
            for pair in range(PAIRS):
                for half, p in enumerate(partner(pair)):
                    for part in range(2):
                        for lane in range(2):
                            at = part * 8 * PITCH + pair * 16 + half * 8
                            o_ref[f, q * 16 + p, v * 2 + part, lane] = stage_ref[lane, pl.ds(at + q, 8, stride=PITCH), :]
            return carry

        lax.fori_loop(0, 8, out_rows, 0)

    each(0, 4, r_arrived)
    zt_fetch.start()
    zb_fetch(0).start()
    zt_fetch.wait()

    def units(unit, carry):
        zb_fetch(unit).wait()

        @pl.when(unit == 3)
        def _():
            each(4, CHUNKS - 1, r_arrived)

        @pl.when(unit < 7)
        def _():
            zb_fetch(unit + 1).start()

        @pl.when(unit >= 4)
        def _():
            each(1, 8, lambda o: tail_copy(unit - 4, o).wait_recv())

        z_unit(unit)
        return carry

    lax.fori_loop(0, 8, units, 0)
    each(0, CHUNKS - 1, lambda c: each(1, 8, lambda o: r_copy(c, o).wait_send()))
    each(0, 4, lambda v: each(1, 8, lambda o: tail_copy(v, o).wait_send()))


def transform(x, sx, sy, sz):
    f32 = jnp.float32
    bf16 = jnp.bfloat16
    dma = pltpu.SemaphoreType.DMA
    hbm = pl.BlockSpec(memory_space=pltpu.HBM)
    _, _, out = pl.pallas_call(
        transform_kernel,
        out_shape=(
            jax.ShapeDtypeStruct((CHUNKS, 16, 2, 128, LANES), f32),
            jax.ShapeDtypeStruct((8, 2, 4, PAIRS, 64, LANES), f32),
            pltpu.VMEM((2, 128, 8, 2, 8, LANES), f32),
        ),
        in_specs=[hbm] * 7,
        out_specs=(hbm, hbm, pl.BlockSpec(memory_space=pltpu.VMEM)),
        scratch_shapes=[
            pltpu.VMEM((RADIX, 1024, LANES), f32),
            pltpu.VMEM((PAIRS, 512, 256), bf16),
            pltpu.VMEM((PAIRS, 512, 256), bf16),
            pltpu.VMEM((256, 512), bf16),
            pltpu.VMEM((16, LANES), f32),
            pltpu.SMEM((512,), f32),
            pltpu.VMEM((1, 256), f32),
            pltpu.VMEM((CHUNKS, 16, 2, 128, LANES), f32),
            pltpu.VMEM((16, 2, 128, LANES), f32),
            pltpu.VMEM((2, 8, PAIRS, 48, LANES), f32),
            pltpu.VMEM((2, 8, 4, PAIRS, 16, LANES), f32),
            pltpu.VMEM((PAIRS, 256, 256), bf16),
            pltpu.VMEM((PAIRS, 256, 256), bf16),
            pltpu.VMEM((2, 16 * PITCH, LANES), f32),
            pltpu.VMEM((128, 256), f32),
            pltpu.VMEM((LANES, LANES), f32),
            dma((8, RADIX)),
            dma((6,)),
            dma,
            dma((2,)),
            dma,
            dma((CHUNKS, 16)),
            dma((CHUNKS, 16)),
            dma((CHUNKS,)),
            dma((CHUNKS, 8)),
            dma((CHUNKS, 8)),
            dma((CHUNKS,)),
            dma((4, 8)),
            dma((4, 8)),
        ],
        compiler_params=pltpu.CompilerParams(
            collective_id=0, has_side_effects=True, vmem_limit_bytes=VMEM_BYTES
        ),
        name="transform",
    )(x, x_tables(), y_tables(), z_table(), sx, sy, sz)
    return jnp.transpose(out, (0, 1, 2, 4, 3, 5)).reshape(2, 128, 64, 256)


def local(tracer, symbol_x, symbol_y, symbol_z):
    x = jnp.transpose(tracer, (0, 2, 3, 1)).reshape(2, 1024, 2048)
    return transform(x, symbol_x.reshape(16, LANES), symbol_y, symbol_z.reshape(1, 256))


def solution(mesh):
    in_specs = (P(None, None, "left", "right"), P(), P(), P())
    out_specs = P(None, "left", "right", None)
    return jax.shard_map(local, mesh=mesh, in_specs=in_specs, out_specs=out_specs, check_vma=False)
```

```python
import jax
import jax.numpy as jnp
import numpy as np
from jax import lax
from jax.experimental import pallas as pl
from jax.experimental.pallas import tpu as pltpu
from jax.sharding import PartitionSpec as P

MESH = pl.DeviceIdType.MESH
RADIX = 16
PAIRS = 8
LANES = 128
CHUNKS = 8
VMEM_BYTES = 44 * 2**20
PITCH = 136
UNROLL = 2


def partner(pair):
    return (0, 8) if pair == 0 else (pair, RADIX - pair)


def split_bf16(table):
    high = table.astype(jnp.bfloat16)
    low = (table - high.astype(np.float32)).astype(jnp.bfloat16)
    return np.asarray(high), np.asarray(low)


def pair_blocks(count):
    inner = count // RADIX
    blocks = np.zeros((PAIRS, 2, 2, inner, inner), np.float64)
    i = np.arange(inner)[:, None]
    q = np.arange(inner)[None, :]
    for pair in range(PAIRS):
        ids = partner(pair)
        for half in range(2):
            angle = 2 * np.pi * ((i * (ids[half] + RADIX * q)) % count) / count
            if pair == 0:
                blocks[pair, half, half] = np.cos(angle) + np.sin(angle)
            else:
                blocks[pair, half, half] = np.cos(angle)
                blocks[pair, half, 1 - half] = np.sin(angle)
    return blocks / np.sqrt(count)


def stacked_tables(table):
    high, low = split_bf16(table.astype(np.float32))
    return np.concatenate([high, low], axis=1)


def x_tables():
    blocks = pair_blocks(2048)
    q = blocks.reshape(PAIRS, 2, 2, 128, 16, 8)
    rows = np.transpose(q, (0, 4, 1, 5, 2, 3))
    return stacked_tables(rows.reshape(PAIRS, 256, 256))


def y_tables():
    blocks = pair_blocks(512)
    v = blocks.reshape(PAIRS, 2, 2, 32, 8, 4)
    full = np.einsum("pabrdv,jk->pdvjabrk", v, np.eye(4))
    return stacked_tables(full.reshape(PAIRS, 256, 256))


def z_table():
    src, zc, j = np.meshgrid(np.arange(8), np.arange(8), np.arange(4), indexing="ij")
    z = (32 * src + 8 * j + zc).reshape(-1)
    k = np.arange(256)
    angle = 2 * np.pi * ((z[:, None] * k[None, :]) % 256) / 256
    table = ((np.cos(angle) + np.sin(angle)) / 16.0).astype(np.float32)
    high, low = split_bf16(table)
    return np.concatenate([high, low], axis=1)


def small_hartley(v):
    n = len(v)
    if n == 1:
        return v
    half = n // 2
    even = small_hartley(v[0::2])
    odd = small_hartley(v[1::2])
    out = [None] * n
    for k in range(half):
        c = float(np.cos(2 * np.pi * k / n))
        s = float(np.sin(2 * np.pi * k / n))
        back = odd[-k % half]
        if k == 0:
            turned = odd[0]
        elif 4 * k == n:
            turned = back
        elif 8 * k == n:
            turned = (odd[k] + back) * c
        elif 8 * k == 3 * n:
            turned = (back - odd[k]) * s
        else:
            turned = odd[k] * c + back * s
        out[k] = even[k] + turned
        out[k + half] = even[k] - turned
    return out


NT = (((1,), (1,)), ((), ()))
TN = (((0,), (0,)), ((), ()))


def radix_step(load, high_ref, low_ref):
    def rows(t, carry):
        zz, g = t // 8, t % 8
        parts = small_hartley(load(zz, g))
        at = pl.ds(pl.multiple_of(zz * 128 + g * 16, 16), 16)
        for pair in range(PAIRS):
            for half, p in enumerate(partner(pair)):
                value = parts[p]
                high = value.astype(jnp.bfloat16)
                low = (value - high.astype(jnp.float32)).astype(jnp.bfloat16)
                lanes = slice(half * LANES, (half + 1) * LANES)
                high_ref[pair, at, lanes] = high
                low_ref[pair, at, lanes] = low
        return carry

    lax.fori_loop(0, 16, rows, 0)


def matmul_step(table_ref, high_ref, low_ref, store):
    def some(i, carry):
        for j in range(UNROLL):
            pair = i * UNROLL + j
            table = table_ref[pair]
            both = lax.dot_general(table, high_ref[pair], NT, preferred_element_type=jnp.float32)
            rest = lax.dot_general(table[:256], low_ref[pair], NT, preferred_element_type=jnp.float32)
            store(pair, both[:256] + both[256:] + rest)
        return carry

    lax.fori_loop(0, PAIRS // UNROLL, some, 0)


def z_core(rows_of, scale_of, write, h_ref, high_ref, low_ref, stage_ref):
    for pair in range(PAIRS):
        for half, u in enumerate(partner(pair)):
            value = jnp.concatenate(rows_of(pair, half), axis=0)
            high = value.astype(jnp.bfloat16)
            low = (value - high.astype(jnp.float32)).astype(jnp.bfloat16)
            lanes = slice(u % 2 * LANES, (u % 2 + 1) * LANES)
            high_ref[u // 2, :, lanes] = high
            low_ref[u // 2, :, lanes] = low

    def some(t, carry):
        both = lax.dot_general(high_ref[t], h_ref[...], TN, preferred_element_type=jnp.float32)
        rest = lax.dot_general(low_ref[t], h_ref[:, :256], TN, preferred_element_type=jnp.float32)
        acc = both[:, :256] + both[:, 256:] + rest
        for i in range(2):
            u = t * 2 + i
            value = acc[i * LANES : (i + 1) * LANES] * scale_of(u)
            for lane in range(2):
                at = pl.ds(pl.multiple_of(u * PITCH, 8), LANES)
                stage_ref[lane, at, :] = value[:, lane * LANES : (lane + 1) * LANES]
        return carry

    lax.fori_loop(0, PAIRS, some, 0)

    def out_rows(q, carry):
        for pair in range(PAIRS):
            for half, p in enumerate(partner(pair)):
                for part in range(2):
                    for lane in range(2):
                        at = part * 8 * PITCH + pair * 16 + half * 8
                        write(q * 16 + p, part, lane, stage_ref[lane, pl.ds(at + q, 8, stride=PITCH), :])
        return carry

    lax.fori_loop(0, 8, out_rows, 0)


def transform_kernel(
    x_hbm, wx_hbm, wy_hbm, h_hbm, sx_hbm, sy_hbm, sz_hbm, l_hbm, r_hbm, o_ref, last_ref, base_ref, level_ref, h_ref,
    x_ref, wx_ref, wy_ref, sx_ref, sy_ref, sz_ref, xo_ref, lb_ref, zb_ref, zt_ref, high_ref, low_ref,
    stage_ref, turn_ref,
    load_sem, table_sem, fetch_sem, zb_sem, zt_sem, last_sem,
    l_send, l_recv, l_own, r_send, r_recv, r_own, tail_send, tail_recv,
):
    left = lax.axis_index("left")
    right = lax.axis_index("right")

    def left_to(o):
        m = 16 - o
        dx, dy, dc = m // 8, m // 2 % 4, m % 2
        return lax.rem(left // 4 + dy, 4) * 4 + lax.rem(left // 2 + dx, 2) * 2 + lax.rem(left + dc, 2)

    def right_to(o):
        m = 8 - o
        dx, dz = m // 4, m % 4
        return lax.rem(right // 2 + dz, 4) * 2 + lax.rem(right + dx, 2)

    def each(first, last, action):
        def one(i, carry):
            action(i)
            return carry

        lax.fori_loop(first, last, one, 0)

    def x_load(c, a):
        two = pl.ds(c % 4 * 2, 2)
        lanes = pl.ds(pl.multiple_of(a * LANES, LANES), LANES)
        return pltpu.make_async_copy(x_hbm.at[c // 4, :, two, lanes], x_tiles.at[a, :, two], load_sem.at[c, a])

    def x_start(c):
        each(0, RADIX, lambda a: x_load(c, a).start())

    wx_load = pltpu.make_async_copy(wx_hbm, wx_ref, table_sem.at[0])
    other_loads = [
        pltpu.make_async_copy(source, target, table_sem.at[1 + i])
        for i, (source, target) in enumerate(
            ((wy_hbm, wy_ref), (h_hbm, h_ref), (sx_hbm, sx_ref), (sy_hbm, sy_ref), (sz_hbm, sz_ref))
        )
    ]

    x_tiles = x_ref.reshape(RADIX, LANES, 8, LANES)
    x_start(0)
    wx_load.start()
    each(1, 4, x_start)
    for load in other_loads:
        load.start()

    barrier = pltpu.get_barrier_semaphore()

    def greet(device):
        pl.semaphore_signal(barrier, inc=1, device_id=device, device_id_type=MESH)

    each(1, 16, lambda o: greet((left_to(o), right)))
    each(1, 8, lambda o: greet((left, right_to(o))))

    def l_copy(c, o):
        to = left_to(o)
        return pltpu.make_async_remote_copy(
            src_ref=xo_ref.at[c, to],
            dst_ref=l_hbm.at[c, left],
            send_sem=l_send.at[c, o],
            recv_sem=l_recv.at[c, o],
            device_id=(to, right),
            device_id_type=MESH,
        )

    def l_keep(c):
        return pltpu.make_async_copy(xo_ref.at[c, left], l_hbm.at[c, left], l_own.at[c])

    yo_ref = xo_ref.reshape(CHUNKS, 8, 4, PAIRS, 16, LANES)

    def r_rows(c):
        return pl.ds(pl.multiple_of((c % 4) * 16, 16), 16)

    def r_copy(c, o):
        to = right_to(o)
        return pltpu.make_async_remote_copy(
            src_ref=yo_ref.at[c, to],
            dst_ref=r_hbm.at[right, c // 4, :, :, r_rows(c)],
            send_sem=r_send.at[c, o],
            recv_sem=r_recv.at[c, o],
            device_id=(left, to),
            device_id_type=MESH,
        )

    def r_keep(c):
        return pltpu.make_async_copy(
            yo_ref.at[c, right], r_hbm.at[right, c // 4, :, :, r_rows(c)], r_own.at[c]
        )

    def tail_copy(v, o):
        to = right_to(o)
        return pltpu.make_async_remote_copy(
            src_ref=yo_ref.at[CHUNKS - 1, to, v],
            dst_ref=zt_ref.at[1, right, v],
            send_sem=tail_send.at[v, o],
            recv_sem=tail_recv.at[v, o],
            device_id=(left, to),
            device_id_type=MESH,
        )

    def last_copy(o):
        to = right_to(o)
        return pltpu.make_async_remote_copy(
            src_ref=yo_ref.at[CHUNKS - 1, to, 3],
            dst_ref=last_ref.at[right, :, 48:64],
            send_sem=tail_send.at[3, o],
            recv_sem=tail_recv.at[3, o],
            device_id=(left, to),
            device_id_type=MESH,
        )

    def x_chunk(c, first_time=False):
        @pl.when(c == 3)
        def _():
            x_start(4)

        @pl.when(c == 4)
        def _():
            each(5, 8, x_start)

        each(0, RADIX, lambda a: x_load(c, a).wait())
        first = (c % 4) * 2

        def load(zz, g):
            rows = pl.ds(g * LANES + first + zz, 16, stride=8)
            return [x_ref[a, rows, :] for a in range(RADIX)]

        def store(pair, value):
            at = pl.ds(pl.multiple_of(pair * 16, 16), 16)
            for zz in range(2):
                xo_ref[c, :, zz, at, :] = value[:, zz * LANES : (zz + 1) * LANES].reshape(16, 16, LANES)

        radix_step(load, high_ref, low_ref)

        if first_time:
            wx_load.wait()

        matmul_step(wx_ref, high_ref, low_ref, store)

    def x_send(c):
        each(1, 16, lambda o: l_copy(c, o).start())
        l_keep(c).start()

    def y_chunk(c):
        l_keep(c).wait()
        each(1, 16, lambda o: l_copy(c, o).wait_recv())
        fetch = pltpu.make_async_copy(l_hbm.at[c], lb_ref, fetch_sem)
        fetch.start()
        each(1, 16, lambda o: l_copy(c, o).wait_send())
        fetch.wait()

        def load(zz, g):
            rows = pl.ds(pl.multiple_of(g * 16, 16), 16)
            return [lb_ref[s, zz, rows, :] for s in range(RADIX)]

        def store(pair, value):
            for zz in range(2):
                yo_ref[c, :, :, pair, zz * 8 : (zz + 1) * 8, :] = value[:, zz * LANES : (zz + 1) * LANES].reshape(
                    8, 4, 8, LANES
                )

        radix_step(load, high_ref, low_ref)
        matmul_step(wy_ref, high_ref, low_ref, store)

        @pl.when(c < CHUNKS - 1)
        def _():
            each(1, 8, lambda o: r_copy(c, o).start())
            r_keep(c).start()

    def prepare_scale():
        turn_ref[...] = jnp.transpose(jnp.broadcast_to(sx_ref[pl.ds(left, 1), :], (LANES, LANES)))
        for pair in range(PAIRS):
            for half, p in enumerate(partner(pair)):
                at = pair * 16 + half * 8
                column = turn_ref[pl.ds(p, 8, stride=16), :]
                for lane in range(2):
                    lanes = slice(lane * LANES, (lane + 1) * LANES)
                    base_ref[at : at + 8, lanes] = column + sz_ref[:, lanes]
        for u in range(16):
            level_ref[u * 8 : u * 8 + 8, :] = jnp.full((8, LANES), sy_ref[right * 64 + 48 + u])

    def r_arrived(c):
        each(1, 8, lambda o: r_copy(c, o).wait_recv())
        r_keep(c).wait()

    def zb_fetch(unit):
        slot = unit % 2
        return pltpu.make_async_copy(
            r_hbm.at[:, unit // 4, unit % 4, :, 0:48], zb_ref.at[slot], zb_sem.at[slot]
        )

    zt_fetch = pltpu.make_async_copy(r_hbm.at[:, 0, :, :, 48:64], zt_ref.at[0], zt_sem)

    def z_unit(unit):
        f, v, slot = unit // 4, unit % 4, unit % 2

        def rows_of(pair, half):
            rows = []
            for src in range(8):
                rows.append(zb_ref[slot, src, pair, pl.ds(half, 24, stride=2), :])
                rows.append(zt_ref[f, src, v, pair, pl.ds(half, 8, stride=2), :])
            return rows

        def scale_of(u):
            return lax.rsqrt(base_ref[...] + sy_ref[right * 64 + v * 16 + u])

        def write(kx, part, lane, value):
            o_ref[f, kx, v * 2 + part, lane] = value

        z_core(rows_of, scale_of, write, h_ref, high_ref, low_ref, stage_ref)

    last_fetch = pltpu.make_async_copy(r_hbm.at[:, 1, 3, :, 0:48], last_ref.at[:, :, 0:48], last_sem)

    def y_step(c):
        y_chunk(c)

        @pl.when(c == CHUNKS - 1)
        def _():
            each(0, 3, lambda v: each(1, 8, lambda o: tail_copy(v, o).start()))
            each(1, 8, lambda o: last_copy(o).start())
            zt_ref[1, right, 0:3] = yo_ref[CHUNKS - 1, right, 0:3]
            last_ref[right, :, 48:64] = yo_ref[CHUNKS - 1, right, 3]

    def z_step(unit):
        @pl.when(unit == 0)
        def _():
            prepare_scale()
            each(0, 4, r_arrived)
            zt_fetch.start()
            zb_fetch(0).start()
            zt_fetch.wait()

        @pl.when(unit == 4)
        def _():
            each(4, CHUNKS - 1, r_arrived)
            zb_fetch(4).start()
            last_fetch.start()

        zb_fetch(unit).wait()

        @pl.when((unit % 4 < 3) & (unit < 6))
        def _():
            zb_fetch(unit + 1).start()

        @pl.when(unit >= 4)
        def _():
            each(1, 8, lambda o: tail_copy(unit - 4, o).wait_recv())

        z_unit(unit)

    def step(i):
        @pl.when(((i >= 2) & (i < 9)) | (i == 13))
        def _():
            y_step(i - 2 - 4 * (i // 13))

        @pl.when((i >= 1) & (i < CHUNKS))
        def _():
            x_chunk(i)

        @pl.when(i < CHUNKS)
        def _():
            x_send(i)

        @pl.when(i == 1)
        def _():
            for load in other_loads:
                load.wait()

        @pl.when(((i >= 9) & (i < 13)) | (i >= 14))
        def _():
            z_step(i - 9 - i // 13)

    x_chunk(0, True)
    pl.semaphore_wait(barrier, 22)
    each(0, 17, step)
    last_fetch.wait()
    each(1, 8, lambda o: last_copy(o).wait())
    each(0, CHUNKS - 1, lambda c: each(1, 8, lambda o: r_copy(c, o).wait_send()))
    each(0, 3, lambda v: each(1, 8, lambda o: tail_copy(v, o).wait_send()))


def transform(x, sx, sy, sz):
    f32 = jnp.float32
    bf16 = jnp.bfloat16
    dma = pltpu.SemaphoreType.DMA
    hbm = pl.BlockSpec(memory_space=pltpu.HBM)
    _, _, out, rest, base, level, table = pl.pallas_call(
        transform_kernel,
        out_shape=(
            jax.ShapeDtypeStruct((CHUNKS, 16, 2, 128, LANES), f32),
            jax.ShapeDtypeStruct((8, 2, 4, PAIRS, 64, LANES), f32),
            pltpu.VMEM((2, 128, 8, 2, 8, LANES), f32),
            pltpu.VMEM((8, PAIRS, 64, LANES), f32),
            pltpu.VMEM((128, 256), f32),
            pltpu.VMEM((128, LANES), f32),
            pltpu.VMEM((256, 512), bf16),
        ),
        in_specs=[hbm] * 7,
        out_specs=(hbm, hbm) + (pl.BlockSpec(memory_space=pltpu.VMEM),) * 5,
        scratch_shapes=[
            pltpu.VMEM((RADIX, 1024, LANES), f32),
            pltpu.VMEM((PAIRS, 512, 256), bf16),
            pltpu.VMEM((PAIRS, 512, 256), bf16),
            pltpu.VMEM((16, LANES), f32),
            pltpu.SMEM((512,), f32),
            pltpu.VMEM((1, 256), f32),
            pltpu.VMEM((CHUNKS, 16, 2, 128, LANES), f32),
            pltpu.VMEM((16, 2, 128, LANES), f32),
            pltpu.VMEM((2, 8, PAIRS, 48, LANES), f32),
            pltpu.VMEM((2, 8, 4, PAIRS, 16, LANES), f32),
            pltpu.VMEM((PAIRS, 256, 256), bf16),
            pltpu.VMEM((PAIRS, 256, 256), bf16),
            pltpu.VMEM((2, 16 * PITCH, LANES), f32),
            pltpu.VMEM((LANES, LANES), f32),
            dma((CHUNKS, RADIX)),
            dma((6,)),
            dma,
            dma((2,)),
            dma,
            dma,
            dma((CHUNKS, 16)),
            dma((CHUNKS, 16)),
            dma((CHUNKS,)),
            dma((CHUNKS, 8)),
            dma((CHUNKS, 8)),
            dma((CHUNKS,)),
            dma((4, 8)),
            dma((4, 8)),
        ],
        compiler_params=pltpu.CompilerParams(
            collective_id=0, has_side_effects=True, vmem_limit_bytes=VMEM_BYTES
        ),
        name="transform",
    )(x, x_tables(), y_tables(), z_table(), sx, sy, sz)
    return finish(out, rest, base, level, table)


def finish_kernel(
    done_ref, last_ref, base_ref, level_ref, h_ref, o_hbm, high_ref, low_ref, stage_ref, out_ref, sem
):
    first = pltpu.make_async_copy(done_ref.at[0], o_hbm.at[0], sem.at[0])
    second = pltpu.make_async_copy(done_ref.at[1, :, 0:6], o_hbm.at[1, :, 0:6], sem.at[1])
    third = pltpu.make_async_copy(out_ref, o_hbm.at[1, :, 6:8], sem.at[2])
    first.start()
    second.start()

    def rows_of(pair, half):
        return [last_ref[src, pair, pl.ds(half, 32, stride=2), :] for src in range(8)]

    def scale_of(u):
        level = level_ref[pl.ds(u * 8, 1), :]
        return lax.rsqrt(base_ref[...] + jnp.concatenate([level, level], axis=1))

    def write(kx, part, lane, value):
        out_ref[kx, part, lane] = value

    z_core(rows_of, scale_of, write, h_ref, high_ref, low_ref, stage_ref)
    third.start()
    first.wait()
    second.wait()
    third.wait()


def finish(done, rest, base, level, table):
    f32 = jnp.float32
    vmem = pl.BlockSpec(memory_space=pltpu.VMEM)
    out = pl.pallas_call(
        finish_kernel,
        out_shape=jax.ShapeDtypeStruct((2, 128, 8, 2, 8, LANES), f32),
        in_specs=[vmem] * 5,
        out_specs=pl.BlockSpec(memory_space=pltpu.HBM),
        scratch_shapes=[
            pltpu.VMEM((PAIRS, 256, 256), jnp.bfloat16),
            pltpu.VMEM((PAIRS, 256, 256), jnp.bfloat16),
            pltpu.VMEM((2, 16 * PITCH, LANES), f32),
            pltpu.VMEM((128, 2, 2, 8, LANES), f32),
            pltpu.SemaphoreType.DMA((3,)),
        ],
        compiler_params=pltpu.CompilerParams(vmem_limit_bytes=16 * 2**20),
        name="finish",
    )(done, rest, base, level, table)
    return jnp.transpose(out, (0, 1, 2, 4, 3, 5)).reshape(2, 128, 64, 256)


def local(tracer, symbol_x, symbol_y, symbol_z):
    x = jnp.transpose(tracer, (0, 2, 3, 1)).reshape(2, 128, 8, 2048)
    return transform(x, symbol_x.reshape(16, LANES), symbol_y, symbol_z.reshape(1, 256))


def solution(mesh):
    in_specs = (P(None, None, "left", "right"), P(), P(), P())
    out_specs = P(None, "left", "right", None)
    return jax.shard_map(local, mesh=mesh, in_specs=in_specs, out_specs=out_specs, check_vma=False)
```
